8 devices in a mesh: data: 1 (over z), row: 2 (over y), col: 2 (over x), core: 2 (over core).
Axes of the slice: x: 2, y: 2, z: 1, core: 2. Of those that a mesh axis runs over, the one named last changes fastest.
Arguments:
- tokens: bfloat16 [2, 1024, 2048], P('data', ('row', 'col', 'core'))
- w_qkv: bfloat16 [2048, 3, 32, 64], replicated
- w_out: bfloat16 [32, 64, 2048], replicated
Outputs:
- output: bfloat16 [2, 1024, 2048], P('data', ('row', 'col', 'core'))
All inputs are finite; a program needn't handle non-finite values.
Results may differ from the reference program's by a relative error of at most 0.00747195.
Values are sent between devices in bfloat16 or wider.
A program may use at most 1 GiB of HBM per device.

```python
import jax
import jax.numpy as jnp
from jax import lax

SEQ = 1024
HEADS = 32
HEAD = 64
BATCH = 2
QUERY_BLOCK = 64

CH = HEADS * HEAD


def setup_inputs(seed: int = 0, part: int = 0) -> dict:
    base_key = jax.random.key(seed)
    tok_key = jax.random.fold_in(jax.random.fold_in(base_key, 1), part)
    qkv_key, out_key = jax.random.split(jax.random.fold_in(base_key, 2))
    tokens = jax.random.normal(tok_key, (BATCH, SEQ, CH), jnp.float32)
    w_qkv = jax.random.normal(qkv_key, (CH, 3, HEADS, HEAD), jnp.float32) * (1.5 * CH ** -0.5)
    out_gain = (SEQ / 160.0) ** 0.5 / 1.5
    w_out = jax.random.normal(out_key, (HEADS, HEAD, CH), jnp.float32) * (out_gain * CH ** -0.5)
    return {"tokens": tokens.astype(jnp.bfloat16), "w_qkv": w_qkv.astype(jnp.bfloat16), "w_out": w_out.astype(jnp.bfloat16)}


def reference(tokens, w_qkv, w_out):
    flat_rows = tokens.reshape(BATCH * SEQ, CH)
    qkv_all = jnp.dot(flat_rows, w_qkv.reshape(CH, 3 * CH), preferred_element_type=jnp.float32).astype(jnp.bfloat16)
    qkv_all = qkv_all.astype(jnp.float32).reshape(BATCH, SEQ, 3, HEADS, HEAD)
    per_head = jnp.transpose(qkv_all, (3, 2, 0, 1, 4))
    logit_scale = HEAD ** -0.5
    num_qblk = SEQ // QUERY_BLOCK

    def one_head(head_qkv):
        queries = head_qkv[0].reshape(BATCH, num_qblk, QUERY_BLOCK, HEAD).transpose(1, 0, 2, 3)
        key_rows = head_qkv[1]
        value_rows = head_qkv[2]

        def one_block(q_blk):
            scores = jnp.einsum("bqd,bkd->bqk", q_blk, key_rows) * logit_scale
            attn_prob = jax.nn.softmax(scores, axis=-1)
            return jnp.einsum("bqk,bkd->bqd", attn_prob, value_rows)

        out_blk = lax.map(one_block, queries)
        return out_blk.transpose(1, 0, 2, 3).reshape(BATCH, SEQ, HEAD)

    heads_out = lax.map(one_head, per_head)
    attn_rows = jnp.transpose(heads_out, (1, 2, 0, 3)).reshape(BATCH * SEQ, CH).astype(jnp.bfloat16)
    y_rows = jnp.dot(attn_rows, w_out.reshape(CH, CH), preferred_element_type=jnp.float32).astype(jnp.bfloat16)
    return y_rows.reshape(BATCH, SEQ, CH)
```

```python
import functools

import jax
import jax.numpy as jnp
from jax import lax
from jax.experimental import pallas as pl
from jax.experimental.pallas import tpu as pltpu
from jax.sharding import PartitionSpec as P

BF = jnp.bfloat16
F32 = jnp.float32
NN = (((1,), (0,)), ((), ()))
NT = (((1,), (1,)), ((), ()))
MESH = pl.DeviceIdType.MESH
LOG2E = 1.4426950408889634
BLOCKS = 8
HALF = 1024
PAIRS = 8
STEPS = 16


def dot(a, b, dims):
    return lax.dot_general(a, b, dims, preferred_element_type=F32)


def kernel(
    x_hbm, wt_hbm, wo_hbm, y_ref,
    xbuf, wq, wk, wv, wo, qz, kbuf, vbuf, acc, m_ref, l_ref, s0, s1, p0, p1, a0, a1, o_own, o_out, o_in, y_acc,
    w_sem, xl_sem, own_send, own_recv, ici_send, ici_recv, rel_send, rel_recv, o_sem,
):
    row, col, core = lax.axis_index("row"), lax.axis_index("col"), lax.axis_index("core")
    x_nbr, y_nbr, mate = {"col": 1 - col}, {"row": 1 - row}, {"core": 1 - core}

    def w_copy(j, i, dst):
        start = pl.multiple_of(j * 2048 + core * HALF + i * 256, 256)
        return pltpu.make_async_copy(wt_hbm.at[pl.ds(start, 256)], dst.at[pl.ds(i * 256, 256)], w_sem.at[j * 4 + i])

    w_copies = [w_copy(j, i, dst) for j, dst in enumerate((wq, wk, wv)) for i in range(4)]
    wo_copy = pltpu.make_async_copy(wo_hbm, wo, w_sem.at[12])
    x_local = pltpu.make_async_copy(x_hbm, xbuf.at[0], xl_sem)
    x_local.start()
    for c in w_copies:
        c.start()

    barrier = pltpu.get_barrier_semaphore()
    for dev in (x_nbr, y_nbr, mate):
        pl.semaphore_signal(barrier, inc=1, device_id=dev, device_id_type=MESH)
    pl.semaphore_wait(barrier, 3)

    def remote(src, dst, send, recv, dev):
        return pltpu.make_async_remote_copy(
            src_ref=src, dst_ref=dst, send_sem=send, recv_sem=recv, device_id=dev, device_id_type=MESH
        )

    to_mate = remote(x_hbm, xbuf.at[1], own_send, own_recv, mate)
    to_mate.start()

    def ici(b, s):
        first = b < 4
        dev = x_nbr if first == (s == 0) else y_nbr
        return remote(
            x_hbm.at[pl.ds(s * 128 + (b % 2) * 64, 64)], xbuf.at[b, pl.ds(s * 128, 64)],
            ici_send.at[b, s], ici_recv.at[b, s], dev,
        )

    sends = [ici(b, s) for b in range(2, 6) for s in range(2)]
    for c in sends:
        c.start()

    def forward(b, s):
        return remote(
            xbuf.at[b, pl.ds(s * 128, 64)], xbuf.at[b + 4, pl.ds(s * 128, 64)],
            ici_send.at[b + 4, s], ici_recv.at[b + 4, s], y_nbr if s == 0 else x_nbr,
        )

    def relay(b, s):
        return remote(
            xbuf.at[b, pl.ds(s * 128, 64)], xbuf.at[b, pl.ds(s * 128 + 64, 64)],
            rel_send.at[b, s], rel_recv.at[b, s], mate,
        )

    def arrived(b, s):
        piece = xbuf.at[b, pl.ds(s * 128, 64)]
        return remote(piece, piece, ici_send.at[b, s], ici_recv.at[b, s], mate)

    qz[...] = jnp.zeros_like(qz)
    acc[...] = jnp.zeros_like(acc)
    l_ref[...] = jnp.zeros_like(l_ref)
    m_ref[...] = jnp.full_like(m_ref, -jnp.inf)

    def query_tile(blk, i):
        q_t = (dot(wq[pl.ds(i * 256, 256), :], xbuf[blk], NT) * 0.125).astype(BF)
        for pair in range(2):
            for s in range(2):
                for h in range(2):
                    piece = q_t[pair * 128 + h * 64 : pair * 128 + h * 64 + 64, s * 128 : s * 128 + 128]
                    lanes = h * 256 + blk * 128
                    qz[(i * 2 + pair) * 2 + s, h * 64 : h * 64 + 64, lanes : lanes + 128] = piece

    x_local.wait()
    for i in range(4):
        w_copies[i].wait()
        query_tile(0, i)
    to_mate.wait_recv()
    for i in range(4):
        query_tile(1, i)
    wo_copy.start()
    for c in w_copies[4:]:
        c.wait()

    def scores(t, s_out):
        s, j = t % 2, t // 2
        keys = kbuf[s * 128 : s * 128 + 128, j * 128 : j * 128 + 128]
        s_out[...] = dot(keys, qz[t], NN)

    def weigh(t, s_in, p_out, a_out):
        sc = s_in[...]
        old = m_ref[t]
        new = jnp.maximum(old, jnp.max(sc, axis=0, keepdims=True))
        p = jnp.exp2((sc - new) * LOG2E)
        scale = jnp.exp2((old - new) * LOG2E)
        l_ref[t] = l_ref[t] * scale + jnp.sum(p, axis=0, keepdims=True)
        m_ref[t] = new
        p_out[...] = p.astype(BF)
        a_out[...] = scale

    def add_values(t, p_in, a_in):
        s, j = t % 2, t // 2
        for h in range(2):
            vals = vbuf[j * 128 + h * 64 : j * 128 + h * 64 + 64, s * 128 : s * 128 + 128]
            lanes = slice(h * 256, h * 256 + 256)
            acc[2 * t + h] = acc[2 * t + h] * a_in[:, lanes] + dot(vals, p_in[:, lanes], NN)

    s_b, p_b, a_b = (s0, s1), (p0, p1), (a0, a1)

    def block(b, carry):
        @pl.when(b >= 2)
        def _():
            for s in range(2):
                relay(b, s).wait_recv()

        for n in range(2):
            kbuf[:, n * 512 : n * 512 + 512] = dot(xbuf[b], wk[n * 512 : n * 512 + 512, :], NT).astype(BF)
        for n in range(2):
            vbuf[n * 512 : n * 512 + 512, :] = dot(wv[n * 512 : n * 512 + 512, :], xbuf[b], NT).astype(BF)

        @pl.when((b >= 1) & (b < BLOCKS - 1))
        def _():
            for s in range(2):
                arrived(b + 1, s).wait_recv()
                relay(b + 1, s).start()

        @pl.when((b >= 1) & (b < 3))
        def _():
            for s in range(2):
                forward(b + 1, s).start()

        scores(0, s0)
        scores(1, s1)
        weigh(0, s0, p0, a0)
        for t in range(STEPS):
            if t + 2 < STEPS:
                scores(t + 2, s_b[t % 2])
            if t + 1 < STEPS:
                weigh(t + 1, s_b[(t + 1) % 2], p_b[(t + 1) % 2], a_b[(t + 1) % 2])
            add_values(t, p_b[t % 2], a_b[t % 2])
        return carry

    lax.fori_loop(0, BLOCKS, block, 0)

    for s in range(2):
        for j in range(PAIRS):
            t = 2 * j + s
            parts = [acc[2 * t + h] / l_ref[t][:, h * 256 : h * 256 + 256] for h in range(2)]
            o_rows = jnp.concatenate(parts, axis=0).T.astype(BF)
            o_own[s * 128 : s * 128 + 128, j * 128 : j * 128 + 128] = o_rows[:128]
            o_out[s * 128 : s * 128 + 128, j * 128 : j * 128 + 128] = o_rows[128:]
    o_copy = remote(o_out, o_in, o_sem.at[0], o_sem.at[1], mate)
    o_copy.start()
    wo_copy.wait()
    mine = pl.multiple_of(core * HALF, HALF)
    theirs = pl.multiple_of((1 - core) * HALF, HALF)
    for n in range(4):
        y_acc[:, n * 512 : n * 512 + 512] = dot(o_own[...], wo[pl.ds(mine, HALF), n * 512 : n * 512 + 512], NN)
    o_copy.wait()
    for n in range(4):
        more = dot(o_in[...], wo[pl.ds(theirs, HALF), n * 512 : n * 512 + 512], NN)
        y_ref[:, n * 512 : n * 512 + 512] = (y_acc[:, n * 512 : n * 512 + 512] + more).astype(BF)

    to_mate.wait_send()
    for c in sends:
        c.wait_send()
    for b in range(2, 4):
        for s in range(2):
            forward(b, s).wait_send()
    for b in range(2, BLOCKS):
        for s in range(2):
            relay(b, s).wait_send()


def solution(mesh):
    tok_spec = P("data", ("row", "col", "core"), None)

    def per_device(tokens, w_qkv, w_out):
        x = tokens.reshape(256, 2048)
        wt = jnp.transpose(w_qkv, (1, 2, 3, 0)).reshape(6144, 2048)
        wo = w_out.reshape(2048, 2048)
        dma = pltpu.SemaphoreType.DMA
        y = pl.pallas_call(
            kernel,
            out_shape=jax.ShapeDtypeStruct((256, 2048), BF),
            in_specs=[pl.BlockSpec(memory_space=pl.ANY)] * 3,
            out_specs=pl.BlockSpec(memory_space=pltpu.VMEM),
            scratch_shapes=[
                pltpu.VMEM((BLOCKS, 256, 2048), BF),
                pltpu.VMEM((HALF, 2048), BF),
                pltpu.VMEM((HALF, 2048), BF),
                pltpu.VMEM((HALF, 2048), BF),
                pltpu.VMEM((2048, 2048), BF),
                pltpu.VMEM((STEPS, 128, 512), BF),
                pltpu.VMEM((256, HALF), BF),
                pltpu.VMEM((HALF, 256), BF),
                pltpu.VMEM((2 * STEPS, 64, 256), F32),
                pltpu.VMEM((STEPS, 1, 512), F32),
                pltpu.VMEM((STEPS, 1, 512), F32),
                pltpu.VMEM((128, 512), F32),
                pltpu.VMEM((128, 512), F32),
                pltpu.VMEM((128, 512), BF),
                pltpu.VMEM((128, 512), BF),
                pltpu.VMEM((1, 512), F32),
                pltpu.VMEM((1, 512), F32),
                pltpu.VMEM((256, HALF), BF),
                pltpu.VMEM((256, HALF), BF),
                pltpu.VMEM((256, HALF), BF),
                pltpu.VMEM((256, 2048), F32),
                dma((13,)),
                dma,
                dma,
                dma,
                dma((BLOCKS, 2)),
                dma((BLOCKS, 2)),
                dma((BLOCKS, 2)),
                dma((BLOCKS, 2)),
                dma((2,)),
            ],
            compiler_params=pltpu.CompilerParams(
                collective_id=0, has_side_effects=True, vmem_limit_bytes=58 * 1024 * 1024
            ),
            name="attention",
        )(x, wt, wo)
        return y.reshape(2, 128, 2048)

    return jax.shard_map(per_device, mesh=mesh, in_specs=(tok_spec, P(), P()), out_specs=tok_spec, check_vma=False)
```

```python
import functools

import jax
import jax.numpy as jnp
from jax import lax
from jax.experimental import pallas as pl
from jax.experimental.pallas import tpu as pltpu
from jax.sharding import PartitionSpec as P

BF = jnp.bfloat16
F32 = jnp.float32
NN = (((1,), (0,)), ((), ()))
NT = (((1,), (1,)), ((), ()))
MESH = pl.DeviceIdType.MESH
LOG2E = 1.4426950408889634
BLOCKS = 8
HALF = 1024
PAIRS = 8
STEPS = 16
AHEAD = 3
LAG = 1
FIRST_PART = 5
PARTS = 2
WIDE = 2048 // PARTS


def dot(a, b, dims):
    return lax.dot_general(a, b, dims, preferred_element_type=F32)


def kernel(
    x_hbm, wt_hbm, wo_hbm, y_ref,
    xbuf, wq, wk, wv, wo, k_acc, v_acc, acc, m_ref, l_ref, o_buf, o_out,
    w_sem, xl_sem, own_send, own_recv, ici_send, ici_recv, rel_send, rel_recv,
    part_send, part_recv, prel_send, prel_recv, o_send, o_recv,
    qz, kbuf, vbuf, *bufs,
):
    s_b, p_b, a_b = bufs[:AHEAD], bufs[AHEAD : AHEAD + LAG + 1], bufs[AHEAD + LAG + 1 :]
    row, col, core = lax.axis_index("row"), lax.axis_index("col"), lax.axis_index("core")
    x_nbr, y_nbr, mate = {"col": 1 - col}, {"row": 1 - row}, {"core": 1 - core}
    mine = pl.multiple_of(core * HALF, HALF)
    theirs = pl.multiple_of((1 - core) * HALF, HALF)

    def w_copy(j, i, dst):
        start = pl.multiple_of(j * 2048 + core * HALF + i * 256, 256)
        return pltpu.make_async_copy(wt_hbm.at[pl.ds(start, 256)], dst.at[pl.ds(i * 256, 256)], w_sem.at[j * 4 + i])

    wq_copies, wk_copies, wv_copies = [[w_copy(j, i, dst) for i in range(4)] for j, dst in enumerate((wq, wk, wv))]
    wo_copies = [
        pltpu.make_async_copy(wo_hbm.at[pl.ds(start, HALF)], wo.at[pl.ds(i * HALF, HALF)], w_sem.at[12 + i])
        for i, start in enumerate((mine, theirs))
    ]
    x_locals = [
        pltpu.make_async_copy(x_hbm.at[pl.ds(i * 64, 64)], xbuf.at[0, pl.ds(i * 64, 64)], xl_sem.at[i])
        for i in range(4)
    ]
    for c in x_locals:
        c.start()
    barrier = pltpu.get_barrier_semaphore()
    for dev in (x_nbr, y_nbr, mate):
        pl.semaphore_signal(barrier, inc=1, device_id=dev, device_id_type=MESH)
    qz[...] = jnp.zeros_like(qz)
    acc[...] = jnp.zeros_like(acc)
    l_ref[...] = jnp.zeros_like(l_ref)
    m_ref[...] = jnp.full_like(m_ref, -jnp.inf)
    for c in x_locals:
        c.wait()
    for c in wq_copies:
        c.start()
    pl.semaphore_wait(barrier, 3)

    def remote(src, dst, send, recv, dev):
        return pltpu.make_async_remote_copy(
            src_ref=src, dst_ref=dst, send_sem=send, recv_sem=recv, device_id=dev, device_id_type=MESH
        )

    def piece(b, s, second=False):
        return xbuf.at[b, pl.ds(s * 128 + (64 if second else 0), 64)]

    def part(b, s, c, second=False):
        return xbuf.at[b, pl.ds(s * 128 + (64 if second else 0), 64), pl.ds(c * WIDE, WIDE)]

    def link_of(b, s):
        return x_nbr if (b < 4) == (s == 0) else y_nbr

    def direct(b, s):
        src = xbuf.at[0, pl.ds(s * 128 + (b % 2) * 64, 64)]
        return remote(src, piece(b, s), ici_send.at[b, s], ici_recv.at[b, s], link_of(b, s))

    def direct_part(b, s, c):
        src = xbuf.at[0, pl.ds(s * 128 + (b % 2) * 64, 64), pl.ds(c * WIDE, WIDE)]
        i = b - FIRST_PART
        return remote(src, part(b, s, c), part_send.at[i, s, c], part_recv.at[i, s, c], link_of(b, s))

    def forward_part(b, s, c):
        i = b + 4 - FIRST_PART
        dev = y_nbr if s == 0 else x_nbr
        return remote(part(b, s, c), part(b + 4, s, c), part_send.at[i, s, c], part_recv.at[i, s, c], dev)

    def relay(b, s):
        return remote(piece(b, s), piece(b, s, True), rel_send.at[b, s], rel_recv.at[b, s], mate)

    def relay_part(b, s, c):
        i = b - FIRST_PART
        return remote(part(b, s, c), part(b, s, c, True), prel_send.at[i, s, c], prel_recv.at[i, s, c], mate)

    def arrived(b, s):
        return remote(piece(b, s), piece(b, s), ici_send.at[b, s], ici_recv.at[b, s], mate)

    def arrived_part(b, s, c):
        i = b - FIRST_PART
        return remote(part(b, s, c), part(b, s, c), part_send.at[i, s, c], part_recv.at[i, s, c], mate)

    to_mate = remote(xbuf.at[0], xbuf.at[1], own_send, own_recv, mate)
    sends = []
    for b, s in ((2, 0), (2, 1), (3, 0), (3, 1), (4, 0), (4, 1), (5, 0), (5, 1)):
        if b == 4 and s == 0:
            to_mate.start()
        if b < FIRST_PART:
            sends.append(direct(b, s))
            sends[-1].start()
        for c in range(PARTS if b >= FIRST_PART else 0):
            sends.append(direct_part(b, s, c))
            sends[-1].start()

    def query_tile(blk, i):
        q_t = (dot(wq[pl.ds(i * 256, 256), :], xbuf[blk], NT) * 0.125).astype(BF)
        for pair in range(2):
            for s in range(2):
                for h in range(2):
                    tile = q_t[pair * 128 + h * 64 : pair * 128 + h * 64 + 64, s * 128 : s * 128 + 128]
                    lanes = h * 256 + blk * 128
                    qz[(i * 2 + pair) * 2 + s, h * 64 : h * 64 + 64, lanes : lanes + 128] = tile

    for i in range(4):
        wq_copies[i].wait()
        for c in (wk_copies + wv_copies)[2 * i : 2 * i + 2]:
            c.start()
        query_tile(0, i)
    to_mate.wait_recv()
    for i in range(4):
        query_tile(1, i)
    for c in wk_copies + wv_copies:
        c.wait()
    for c in wo_copies:
        c.start()

    def scores(t, s_out):
        s, j = t % 2, t // 2
        s_out[...] = dot(kbuf[s * 128 : s * 128 + 128, j * 128 : j * 128 + 128], qz[t], NN)

    def weigh(t, s_in, p_out, a_out):
        sc = s_in[...]
        old = m_ref[t]
        new = jnp.maximum(old, jnp.max(sc, axis=0, keepdims=True))
        p = jnp.exp2((sc - new) * LOG2E)
        scale = jnp.exp2((old - new) * LOG2E)
        l_ref[t] = l_ref[t] * scale + jnp.sum(p.reshape(16, 8, 512), axis=0)
        m_ref[t] = new
        p_out[...] = p.astype(BF)
        a_out[...] = scale

    def add_values(t, p_in, a_in):
        s, j = t % 2, t // 2
        for h in range(2):
            vals = vbuf[j * 128 + h * 64 : j * 128 + h * 64 + 64, s * 128 : s * 128 + 128]
            lanes = slice(h * 256, h * 256 + 256)
            acc[2 * t + h] = acc[2 * t + h] * a_in[:, lanes] + dot(vals, p_in[:, lanes], NN)

    def attend(order, hooks):
        def weigh_step(i):
            weigh(order[i], s_b[i % AHEAD], p_b[i % (LAG + 1)], a_b[i % (LAG + 1)])

        for i in range(AHEAD):
            scores(order[i], s_b[i])
        for i in range(LAG):
            weigh_step(i)
        for i, t in enumerate(order):
            if i + LAG < STEPS:
                weigh_step(i + LAG)
            if i + AHEAD < STEPS:
                scores(order[i + AHEAD], s_b[i % AHEAD])
            add_values(t, p_b[i % (LAG + 1)], a_b[i % (LAG + 1)])
            if i in hooks:
                hooks[i]()

    def pass_on(b, c):
        for s in range(2):
            arrived_part(b, s, c).wait_recv()
            relay_part(b, s, c).start()

    def block(b, carry):
        @pl.when(b >= 2)
        def _():
            for s in range(2):
                relay(b, s).wait_recv()

        for n in range(2):
            kbuf[:, n * 512 : n * 512 + 512] = dot(xbuf[b], wk[n * 512 : n * 512 + 512, :], NT).astype(BF)
        for n in range(2):
            vbuf[n * 512 : n * 512 + 512, :] = dot(wv[n * 512 : n * 512 + 512, :], xbuf[b], NT).astype(BF)

        @pl.when((b >= 1) & (b < FIRST_PART - 1))
        def _():
            for s in range(2):
                arrived(b + 1, s).wait_recv()
                relay(b + 1, s).start()

        @pl.when((b >= 1) & (b < 3))
        def _():
            for c in range(PARTS):
                for s in range(2):
                    forward_part(b + 1, s, c).start()

        @pl.when(b == FIRST_PART - 1)
        def _():
            pass_on(FIRST_PART, 0)

        attend(list(range(STEPS)), {})
        return carry

    lax.fori_loop(0, FIRST_PART, block, 0)

    def project_part(b, c):
        cols = slice(c * WIDE, c * WIDE + WIDE)
        x_part = xbuf[b, :, cols]
        for n in range(2):
            lanes = slice(n * 512, n * 512 + 512)
            k_new = dot(x_part, wk[lanes, cols], NT)
            v_new = dot(wv[lanes, cols], x_part, NT)
            if c > 0:
                k_new += k_acc[:, lanes]
                v_new += v_acc[lanes, :]
            if c < PARTS - 1:
                k_acc[:, lanes] = k_new
                v_acc[lanes, :] = v_new
            else:
                kbuf[:, lanes] = k_new.astype(BF)
                vbuf[lanes, :] = v_new.astype(BF)

    def project_parts(b):
        for c in range(PARTS):
            if c + 1 < PARTS:
                pass_on(b, c + 1)
            for s in range(2):
                relay_part(b, s, c).wait_recv()
            project_part(b, c)

    for b in range(FIRST_PART, BLOCKS):
        project_parts(b)
        if b < BLOCKS - 1:
            pass_on(b + 1, 0)
            attend(list(range(STEPS)), {})

    def o_copy(s):
        dst = o_buf.at[pl.ds(s * 128, 128), pl.ds(HALF, HALF)]
        return remote(o_out.at[pl.ds(s * 128, 128)], dst, o_send.at[s], o_recv.at[s], mate)

    def finish(s):
        for j in range(PAIRS):
            t = 2 * j + s
            total = jnp.sum(l_ref[t], axis=0, keepdims=True)
            parts = [acc[2 * t + h] / total[:, h * 256 : h * 256 + 256] for h in range(2)]
            o_rows = jnp.concatenate(parts, axis=0).T.astype(BF)
            o_out[s * 128 : s * 128 + 128, j * 128 : j * 128 + 128] = o_rows[128:]
            o_buf[s * 128 : s * 128 + 128, j * 128 : j * 128 + 128] = o_rows[:128]
        o_copy(s).start()

    attend([2 * j + s for s in range(2) for j in range(PAIRS)], {STEPS // 2 - 1: lambda: finish(0)})
    finish(1)
    for c in wo_copies:
        c.wait()
    for s in range(2):
        o_copy(s).wait_recv()
        for n in range(4):
            lanes = slice(n * 512, n * 512 + 512)
            y_ref[s * 128 : s * 128 + 128, lanes] = dot(o_buf[s * 128 : s * 128 + 128, :], wo[:, lanes], NN).astype(BF)

    to_mate.wait_send()
    for c in sends:
        c.wait_send()
    for s in range(2):
        o_copy(s).wait_send()
        for b in range(2, FIRST_PART):
            relay(b, s).wait_send()
        for c in range(PARTS):
            for b in range(2, 4):
                forward_part(b, s, c).wait_send()
            for b in range(FIRST_PART, BLOCKS):
                relay_part(b, s, c).wait_send()


def solution(mesh):
    tok_spec = P("data", ("row", "col", "core"), None)

    def per_device(tokens, w_qkv, w_out):
        x = tokens.reshape(256, 2048)
        wt = jnp.transpose(w_qkv, (1, 2, 3, 0)).reshape(6144, 2048)
        wo = w_out.reshape(2048, 2048)
        dma = pltpu.SemaphoreType.DMA
        local = [
            pltpu.VMEM((STEPS, 128, 512), BF),
            pltpu.VMEM((256, HALF), BF),
            pltpu.VMEM((HALF, 256), BF),
            *[pltpu.VMEM((128, 512), F32)] * AHEAD,
            *[pltpu.VMEM((128, 512), BF)] * (LAG + 1),
            *[pltpu.VMEM((1, 512), F32)] * (LAG + 1),
        ]
        y = pl.pallas_call(
            lambda *refs: pl.run_scoped(functools.partial(kernel, *refs), *local),
            out_shape=jax.ShapeDtypeStruct((256, 2048), BF),
            in_specs=[pl.BlockSpec(memory_space=pl.ANY)] * 3,
            out_specs=pl.BlockSpec(memory_space=pltpu.VMEM),
            scratch_shapes=[
                pltpu.VMEM((BLOCKS, 256, 2048), BF),
                pltpu.VMEM((HALF, 2048), BF),
                pltpu.VMEM((HALF, 2048), BF),
                pltpu.VMEM((HALF, 2048), BF),
                pltpu.VMEM((2048, 2048), BF),
                pltpu.VMEM((256, HALF), F32),
                pltpu.VMEM((HALF, 256), F32),
                pltpu.VMEM((2 * STEPS, 64, 256), F32),
                pltpu.VMEM((STEPS, 1, 512), F32),
                pltpu.VMEM((STEPS, 8, 512), F32),
                pltpu.VMEM((256, 2048), BF),
                pltpu.VMEM((256, HALF), BF),
                dma((14,)),
                dma((4,)),
                dma,
                dma,
                dma((FIRST_PART, 2)),
                dma((FIRST_PART, 2)),
                dma((FIRST_PART, 2)),
                dma((FIRST_PART, 2)),
                dma((BLOCKS - FIRST_PART, 2, PARTS)),
                dma((BLOCKS - FIRST_PART, 2, PARTS)),
                dma((BLOCKS - FIRST_PART, 2, PARTS)),
                dma((BLOCKS - FIRST_PART, 2, PARTS)),
                dma((2,)),
                dma((2,)),
            ],
            compiler_params=pltpu.CompilerParams(
                collective_id=0, has_side_effects=True, vmem_limit_bytes=52 * 1024 * 1024
            ),
            name="attention",
        )(x, wt, wo)
        return y.reshape(2, 128, 2048)

    return jax.shard_map(per_device, mesh=mesh, in_specs=(tok_spec, P(), P()), out_specs=tok_spec, check_vma=False)
```

```python
import functools

import jax
import jax.numpy as jnp
from jax import lax
from jax.experimental import pallas as pl
from jax.experimental.pallas import tpu as pltpu
from jax.sharding import PartitionSpec as P

BF = jnp.bfloat16
F32 = jnp.float32
NN = (((1,), (0,)), ((), ()))
NT = (((1,), (1,)), ((), ()))
MESH = pl.DeviceIdType.MESH
LOG2E = 1.4426950408889634
BLOCKS = 8
HALF = 1024
PAIRS = 8
STEPS = 16
AHEAD = 3
LAG = 1
FIRST_PART = 6
COLS = (0, 1024, 2048)
PARTS = len(COLS) - 1


def dot(a, b, dims):
    return lax.dot_general(a, b, dims, preferred_element_type=F32)


def kernel(
    x_hbm, wt_hbm, wo_hbm, y_ref,
    xbuf, wq, wk, wv, wo, k_acc, v_acc, acc, m_ref, l_ref, o_buf, o_out, y_acc,
    w_sem, xl_sem, own_send, own_recv, ici_send, ici_recv, rel_send, rel_recv,
    part_send, part_recv, prel_send, prel_recv, o_send, o_recv,
    qz, kbuf, vbuf, *bufs,
):
    s_b, p_b, a_b = bufs[:AHEAD], bufs[AHEAD : AHEAD + LAG + 1], bufs[AHEAD + LAG + 1 :]
    row, col, core = lax.axis_index("row"), lax.axis_index("col"), lax.axis_index("core")
    x_nbr, y_nbr, mate = {"col": 1 - col}, {"row": 1 - row}, {"core": 1 - core}
    mine = pl.multiple_of(core * HALF, HALF)
    theirs = pl.multiple_of((1 - core) * HALF, HALF)

    def w_copy(j, i, dst):
        start = pl.multiple_of(j * 2048 + core * HALF + i * 256, 256)
        return pltpu.make_async_copy(wt_hbm.at[pl.ds(start, 256)], dst.at[pl.ds(i * 256, 256)], w_sem.at[j * 4 + i])

    wq_copies, wk_copies, wv_copies = [[w_copy(j, i, dst) for i in range(4)] for j, dst in enumerate((wq, wk, wv))]
    wo_copies = [
        pltpu.make_async_copy(wo_hbm.at[pl.ds(start, HALF)], wo.at[pl.ds(i * HALF, HALF)], w_sem.at[12 + i])
        for i, start in enumerate((mine, theirs))
    ]
    x_locals = [
        pltpu.make_async_copy(x_hbm.at[pl.ds(i * 64, 64)], xbuf.at[0, pl.ds(i * 64, 64)], xl_sem.at[i])
        for i in range(4)
    ]
    for c in x_locals:
        c.start()
    barrier = pltpu.get_barrier_semaphore()
    for dev in (x_nbr, y_nbr, mate):
        pl.semaphore_signal(barrier, inc=1, device_id=dev, device_id_type=MESH)
    qz[...] = jnp.zeros_like(qz)
    acc[...] = jnp.zeros_like(acc)
    l_ref[...] = jnp.zeros_like(l_ref)
    m_ref[...] = jnp.full_like(m_ref, -jnp.inf)
    for c in x_locals:
        c.wait()
    for c in wq_copies:
        c.start()
    pl.semaphore_wait(barrier, 3)

    def remote(src, dst, send, recv, dev):
        return pltpu.make_async_remote_copy(
            src_ref=src, dst_ref=dst, send_sem=send, recv_sem=recv, device_id=dev, device_id_type=MESH
        )

    def piece(b, s, second=False):
        return xbuf.at[b, pl.ds(s * 128 + (64 if second else 0), 64)]

    def part(b, s, c, second=False):
        return xbuf.at[b, pl.ds(s * 128 + (64 if second else 0), 64), pl.ds(COLS[c], COLS[c + 1] - COLS[c])]

    def link_of(b, s):
        return x_nbr if (b < 4) == (s == 0) else y_nbr

    def direct(b, s):
        src = xbuf.at[0, pl.ds(s * 128 + (b % 2) * 64, 64)]
        return remote(src, piece(b, s), ici_send.at[b, s], ici_recv.at[b, s], link_of(b, s))

    def direct_part(b, s, c):
        src = xbuf.at[0, pl.ds(s * 128 + (b % 2) * 64, 64), pl.ds(COLS[c], COLS[c + 1] - COLS[c])]
        i = b - FIRST_PART
        return remote(src, part(b, s, c), part_send.at[i, s, c], part_recv.at[i, s, c], link_of(b, s))

    def forward_part(b, s, c):
        i = b + 4 - FIRST_PART
        dev = y_nbr if s == 0 else x_nbr
        return remote(part(b, s, c), part(b + 4, s, c), part_send.at[i, s, c], part_recv.at[i, s, c], dev)

    def relay(b, s):
        return remote(piece(b, s), piece(b, s, True), rel_send.at[b, s], rel_recv.at[b, s], mate)

    def relay_part(b, s, c):
        i = b - FIRST_PART
        return remote(part(b, s, c), part(b, s, c, True), prel_send.at[i, s, c], prel_recv.at[i, s, c], mate)

    def arrived(b, s):
        return remote(piece(b, s), piece(b, s), ici_send.at[b, s], ici_recv.at[b, s], mate)

    def arrived_part(b, s, c):
        i = b - FIRST_PART
        return remote(part(b, s, c), part(b, s, c), part_send.at[i, s, c], part_recv.at[i, s, c], mate)

    to_mate = remote(xbuf.at[0], xbuf.at[1], own_send, own_recv, mate)
    sends = []
    for b, s in ((2, 0), (2, 1), (3, 0), (3, 1), (4, 0), (4, 1), (5, 0), (5, 1)):
        if b == 4 and s == 0:
            to_mate.start()
        if b < FIRST_PART:
            sends.append(direct(b, s))
            sends[-1].start()
        for c in range(PARTS if b >= FIRST_PART else 0):
            sends.append(direct_part(b, s, c))
            sends[-1].start()

    def query_tile(blk, i):
        q_t = (dot(wq[pl.ds(i * 256, 256), :], xbuf[blk], NT) * 0.125).astype(BF)
        for pair in range(2):
            for s in range(2):
                for h in range(2):
                    tile = q_t[pair * 128 + h * 64 : pair * 128 + h * 64 + 64, s * 128 : s * 128 + 128]
                    lanes = h * 256 + blk * 128
                    qz[(i * 2 + pair) * 2 + s, h * 64 : h * 64 + 64, lanes : lanes + 128] = tile

    for i in range(4):
        wq_copies[i].wait()
        for c in (wk_copies + wv_copies)[2 * i : 2 * i + 2]:
            c.start()
        query_tile(0, i)
    to_mate.wait_recv()
    for i in range(4):
        query_tile(1, i)
    for c in wk_copies + wv_copies:
        c.wait()
    for c in wo_copies:
        c.start()

    def scores(t, s_out):
        s, j = t % 2, t // 2
        s_out[...] = dot(kbuf[s * 128 : s * 128 + 128, j * 128 : j * 128 + 128], qz[t], NN)

    def weigh(t, s_in, p_out, a_out):
        sc = s_in[...]
        old = m_ref[t]
        new = jnp.maximum(old, jnp.max(sc, axis=0, keepdims=True))
        p = jnp.exp2((sc - new) * LOG2E)
        scale = jnp.exp2((old - new) * LOG2E)
        l_ref[t] = l_ref[t] * scale + jnp.sum(p.reshape(16, 8, 512), axis=0)
        m_ref[t] = new
        p_out[...] = p.astype(BF)
        a_out[...] = scale

    def add_values(t, p_in, a_in):
        s, j = t % 2, t // 2
        for h in range(2):
            vals = vbuf[j * 128 + h * 64 : j * 128 + h * 64 + 64, s * 128 : s * 128 + 128]
            lanes = slice(h * 256, h * 256 + 256)
            acc[2 * t + h] = acc[2 * t + h] * a_in[:, lanes] + dot(vals, p_in[:, lanes], NN)

    def attend(order, hooks):
        def weigh_step(i):
            weigh(order[i], s_b[i % AHEAD], p_b[i % (LAG + 1)], a_b[i % (LAG + 1)])

        for i in range(AHEAD):
            scores(order[i], s_b[i])
        for i in range(LAG):
            weigh_step(i)
        for i, t in enumerate(order):
            if i + LAG < STEPS:
                weigh_step(i + LAG)
            if i + AHEAD < STEPS:
                scores(order[i + AHEAD], s_b[i % AHEAD])
            add_values(t, p_b[i % (LAG + 1)], a_b[i % (LAG + 1)])
            if i in hooks:
                hooks[i]()

    def pass_on(b, c):
        for s in range(2):
            arrived_part(b, s, c).wait_recv()
            relay_part(b, s, c).start()

    def whole_block(b):
        @pl.when(b >= 2)
        def _():
            for s in range(2):
                relay(b, s).wait_recv()

        for n in range(2):
            kbuf[:, n * 512 : n * 512 + 512] = dot(xbuf[b], wk[n * 512 : n * 512 + 512, :], NT).astype(BF)
        for n in range(2):
            vbuf[n * 512 : n * 512 + 512, :] = dot(wv[n * 512 : n * 512 + 512, :], xbuf[b], NT).astype(BF)

        @pl.when((b >= 1) & (b < FIRST_PART - 1))
        def _():
            for s in range(2):
                arrived(b + 1, s).wait_recv()
                relay(b + 1, s).start()

        @pl.when((b >= 1) & (b < 3))
        def _():
            for c in range(PARTS):
                for s in range(2):
                    forward_part(b + 1, s, c).start()

        @pl.when(b == FIRST_PART - 1)
        def _():
            pass_on(FIRST_PART, 0)

    def project_part(b, c):
        cols = slice(COLS[c], COLS[c + 1])
        x_part = xbuf[b, :, cols]
        for n in range(2):
            lanes = slice(n * 512, n * 512 + 512)
            k_new = dot(x_part, wk[lanes, cols], NT)
            v_new = dot(wv[lanes, cols], x_part, NT)
            if c > 0:
                k_new += k_acc[:, lanes]
                v_new += v_acc[lanes, :]
            if c < PARTS - 1:
                k_acc[:, lanes] = k_new
                v_acc[lanes, :] = v_new
            else:
                kbuf[:, lanes] = k_new.astype(BF)
                vbuf[lanes, :] = v_new.astype(BF)

    def part_block(b):
        for c in range(PARTS):
            if c + 1 < PARTS:
                pass_on(b, c + 1)
            for s in range(2):
                relay_part(b, s, c).wait_recv()
            project_part(b, c)

    def block(b, carry):
        @pl.when(b < FIRST_PART)
        def _():
            whole_block(b)

        @pl.when(b >= FIRST_PART)
        def _():
            part_block(b)
            pass_on(b + 1, 0)

        attend(list(range(STEPS)), {})
        return carry

    lax.fori_loop(0, BLOCKS - 1, block, 0)
    part_block(BLOCKS - 1)

    def o_copy(s):
        dst = o_buf.at[pl.ds(s * 128, 128), pl.ds(HALF, HALF)]
        return remote(o_out.at[pl.ds(s * 128, 128)], dst, o_send.at[s], o_recv.at[s], mate)

    def finish(s):
        for j in range(PAIRS):
            t = 2 * j + s
            total = jnp.sum(l_ref[t], axis=0, keepdims=True)
            parts = [acc[2 * t + h] / total[:, h * 256 : h * 256 + 256] for h in range(2)]
            o_rows = jnp.concatenate(parts, axis=0).T.astype(BF)
            o_out[s * 128 : s * 128 + 128, j * 128 : j * 128 + 128] = o_rows[128:]
            o_buf[s * 128 : s * 128 + 128, j * 128 : j * 128 + 128] = o_rows[:128]
        o_copy(s).start()

    for c in wo_copies:
        c.wait()

    def own_share(s, n):
        rows, lanes = slice(s * 128, s * 128 + 128), slice(n * 512, n * 512 + 512)
        y_acc[rows, lanes] = dot(o_buf[rows, :HALF], wo[:HALF, lanes], NN)

    def other_share(s, n):
        rows, lanes = slice(s * 128, s * 128 + 128), slice(n * 512, n * 512 + 512)
        y_ref[rows, lanes] = (y_acc[rows, lanes] + dot(o_buf[rows, HALF:], wo[HALF:, lanes], NN)).astype(BF)

    hooks = {PAIRS - 1: lambda: finish(0)}
    for n in range(4):
        hooks[PAIRS + 1 + 2 * n] = functools.partial(own_share, 0, n)
    attend([2 * j + s for s in range(2) for j in range(PAIRS)], hooks)
    finish(1)
    o_copy(0).wait_recv()
    for n in range(4):
        own_share(1, n)
    for n in range(4):
        other_share(0, n)
    o_copy(1).wait_recv()
    for n in range(4):
        other_share(1, n)

    to_mate.wait_send()
    for c in sends:
        c.wait_send()
    for s in range(2):
        o_copy(s).wait_send()
        for b in range(2, FIRST_PART):
            relay(b, s).wait_send()
        for c in range(PARTS):
            for b in range(2, 4):
                forward_part(b, s, c).wait_send()
            for b in range(FIRST_PART, BLOCKS):
                relay_part(b, s, c).wait_send()


def solution(mesh):
    tok_spec = P("data", ("row", "col", "core"), None)

    def per_device(tokens, w_qkv, w_out):
        x = tokens.reshape(256, 2048)
        wt = jnp.transpose(w_qkv, (1, 2, 3, 0)).reshape(6144, 2048)
        wo = w_out.reshape(2048, 2048)
        dma = pltpu.SemaphoreType.DMA
        local = [
            pltpu.VMEM((STEPS, 128, 512), BF),
            pltpu.VMEM((256, HALF), BF),
            pltpu.VMEM((HALF, 256), BF),
            *[pltpu.VMEM((128, 512), F32)] * AHEAD,
            *[pltpu.VMEM((128, 512), BF)] * (LAG + 1),
            *[pltpu.VMEM((1, 512), F32)] * (LAG + 1),
        ]
        y = pl.pallas_call(
            lambda *refs: pl.run_scoped(functools.partial(kernel, *refs), *local),
            out_shape=jax.ShapeDtypeStruct((256, 2048), BF),
            in_specs=[pl.BlockSpec(memory_space=pl.ANY)] * 3,
            out_specs=pl.BlockSpec(memory_space=pltpu.VMEM),
            scratch_shapes=[
                pltpu.VMEM((BLOCKS, 256, 2048), BF),
                pltpu.VMEM((HALF, 2048), BF),
                pltpu.VMEM((HALF, 2048), BF),
                pltpu.VMEM((HALF, 2048), BF),
                pltpu.VMEM((2048, 2048), BF),
                pltpu.VMEM((256, HALF), F32),
                pltpu.VMEM((HALF, 256), F32),
                pltpu.VMEM((2 * STEPS, 64, 256), F32),
                pltpu.VMEM((STEPS, 1, 512), F32),
                pltpu.VMEM((STEPS, 8, 512), F32),
                pltpu.VMEM((256, 2048), BF),
                pltpu.VMEM((256, HALF), BF),
                pltpu.VMEM((256, 2048), F32),
                dma((14,)),
                dma((4,)),
                dma,
                dma,
                dma((FIRST_PART, 2)),
                dma((FIRST_PART, 2)),
                dma((FIRST_PART, 2)),
                dma((FIRST_PART, 2)),
                dma((BLOCKS - FIRST_PART, 2, PARTS)),
                dma((BLOCKS - FIRST_PART, 2, PARTS)),
                dma((BLOCKS - FIRST_PART, 2, PARTS)),
                dma((BLOCKS - FIRST_PART, 2, PARTS)),
                dma((2,)),
                dma((2,)),
            ],
            compiler_params=pltpu.CompilerParams(
                collective_id=0, has_side_effects=True, vmem_limit_bytes=52 * 1024 * 1024
            ),
            name="attention",
        )(x, wt, wo)
        return y.reshape(2, 128, 2048)

    return jax.shard_map(per_device, mesh=mesh, in_specs=(tok_spec, P(), P()), out_specs=tok_spec, check_vma=False)
```

```python
import functools

import jax
import jax.numpy as jnp
from jax import lax
from jax.experimental import pallas as pl
from jax.experimental.pallas import tpu as pltpu
from jax.sharding import PartitionSpec as P

BF = jnp.bfloat16
F32 = jnp.float32
NN = (((1,), (0,)), ((), ()))
NT = (((1,), (1,)), ((), ()))
MESH = pl.DeviceIdType.MESH
LOG2E = 1.4426950408889634
BLOCKS = 8
HALF = 1024
PAIRS = 8
STEPS = 16
AHEAD = 3
LAG = 1
FIRST_PART = 6
COLS = (0, 1024, 2048)
PARTS = len(COLS) - 1


def dot(a, b, dims):
    return lax.dot_general(a, b, dims, preferred_element_type=F32)


def kernel(
    x_hbm, wt_hbm, wo_hbm, y_ref,
    xbuf, wq, wk, wv, wo, k_acc, v_acc, acc, m_ref, l_ref, o_buf, o_out, y_acc,
    w_sem, xl_sem, own_send, own_recv, ici_send, ici_recv, rel_send, rel_recv,
    part_send, part_recv, prel_send, prel_recv, o_send, o_recv,
    qz, kbuf, vbuf, *bufs,
):
    s_b, p_b, a_b = bufs[:AHEAD], bufs[AHEAD : AHEAD + LAG + 1], bufs[AHEAD + LAG + 1 :]
    row, col, core = lax.axis_index("row"), lax.axis_index("col"), lax.axis_index("core")
    x_nbr, y_nbr, mate = {"col": 1 - col}, {"row": 1 - row}, {"core": 1 - core}
    mine = pl.multiple_of(core * HALF, HALF)
    theirs = pl.multiple_of((1 - core) * HALF, HALF)

    def w_copy(j, i, dst):
        start = pl.multiple_of(j * 2048 + core * HALF + i * 256, 256)
        return pltpu.make_async_copy(wt_hbm.at[pl.ds(start, 256)], dst.at[pl.ds(i * 256, 256)], w_sem.at[j * 4 + i])

    wq_copies, wk_copies, wv_copies = [[w_copy(j, i, dst) for i in range(4)] for j, dst in enumerate((wq, wk, wv))]
    wo_copies = [
        pltpu.make_async_copy(wo_hbm.at[pl.ds(start, HALF)], wo.at[pl.ds(i * HALF, HALF)], w_sem.at[12 + i])
        for i, start in enumerate((mine, theirs))
    ]
    x_locals = [
        pltpu.make_async_copy(x_hbm.at[pl.ds(i * 64, 64)], xbuf.at[0, pl.ds(i * 64, 64)], xl_sem.at[i])
        for i in range(4)
    ]
    for c in x_locals:
        c.start()
    barrier = pltpu.get_barrier_semaphore()
    for dev in (x_nbr, y_nbr, mate):
        pl.semaphore_signal(barrier, inc=1, device_id=dev, device_id_type=MESH)
    qz[...] = jnp.zeros_like(qz)
    acc[...] = jnp.zeros_like(acc)
    l_ref[...] = jnp.zeros_like(l_ref)
    m_ref[...] = jnp.full_like(m_ref, -jnp.inf)
    for c in x_locals:
        c.wait()
    for c in wq_copies:
        c.start()
    pl.semaphore_wait(barrier, 3)

    def remote(src, dst, send, recv, dev):
        return pltpu.make_async_remote_copy(
            src_ref=src, dst_ref=dst, send_sem=send, recv_sem=recv, device_id=dev, device_id_type=MESH
        )

    def piece(b, s, second=False):
        return xbuf.at[b, pl.ds(s * 128 + (64 if second else 0), 64)]

    def part(b, s, c, second=False):
        return xbuf.at[b, pl.ds(s * 128 + (64 if second else 0), 64), pl.ds(COLS[c], COLS[c + 1] - COLS[c])]

    def link_of(b, s):
        return x_nbr if (b < 4) == (s == 0) else y_nbr

    def direct(b, s):
        src = xbuf.at[0, pl.ds(s * 128 + (b % 2) * 64, 64)]
        return remote(src, piece(b, s), ici_send.at[b, s], ici_recv.at[b, s], link_of(b, s))

    def direct_part(b, s, c):
        src = xbuf.at[0, pl.ds(s * 128 + (b % 2) * 64, 64), pl.ds(COLS[c], COLS[c + 1] - COLS[c])]
        i = b - FIRST_PART
        return remote(src, part(b, s, c), part_send.at[i, s, c], part_recv.at[i, s, c], link_of(b, s))

    def forward_part(b, s, c):
        i = b + 4 - FIRST_PART
        dev = y_nbr if s == 0 else x_nbr
        return remote(part(b, s, c), part(b + 4, s, c), part_send.at[i, s, c], part_recv.at[i, s, c], dev)

    def relay(b, s):
        return remote(piece(b, s), piece(b, s, True), rel_send.at[b, s], rel_recv.at[b, s], mate)

    def relay_part(b, s, c):
        i = b - FIRST_PART
        return remote(part(b, s, c), part(b, s, c, True), prel_send.at[i, s, c], prel_recv.at[i, s, c], mate)

    def arrived(b, s):
        return remote(piece(b, s), piece(b, s), ici_send.at[b, s], ici_recv.at[b, s], mate)

    def arrived_part(b, s, c):
        i = b - FIRST_PART
        return remote(part(b, s, c), part(b, s, c), part_send.at[i, s, c], part_recv.at[i, s, c], mate)

    to_mate = remote(xbuf.at[0], xbuf.at[1], own_send, own_recv, mate)
    sends = []
    for b, s in ((2, 0), (2, 1), (3, 0), (3, 1), (4, 0), (4, 1), (5, 0), (5, 1)):
        if b == 4 and s == 0:
            to_mate.start()
        if b < FIRST_PART:
            sends.append(direct(b, s))
            sends[-1].start()
        for c in range(PARTS if b >= FIRST_PART else 0):
            sends.append(direct_part(b, s, c))
            sends[-1].start()

    def query_tile(blk, i):
        q_t = (dot(wq[pl.ds(i * 256, 256), :], xbuf[blk], NT) * 0.125).astype(BF)
        for pair in range(2):
            for s in range(2):
                for h in range(2):
                    tile = q_t[pair * 128 + h * 64 : pair * 128 + h * 64 + 64, s * 128 : s * 128 + 128]
                    lanes = h * 256 + blk * 128
                    qz[(i * 2 + pair) * 2 + s, h * 64 : h * 64 + 64, lanes : lanes + 128] = tile

    for i in range(4):
        wq_copies[i].wait()
        for c in (wk_copies + wv_copies)[2 * i : 2 * i + 2]:
            c.start()
        query_tile(0, i)
    to_mate.wait_recv()
    for i in range(4):
        query_tile(1, i)
    for c in wk_copies + wv_copies:
        c.wait()
    for c in wo_copies:
        c.start()

    def scores(t, s_out):
        s, j = t % 2, t // 2
        s_out[...] = dot(kbuf[s * 128 : s * 128 + 128, j * 128 : j * 128 + 128], qz[t], NN)

    def weigh(t, s_in, p_out, a_out):
        sc = s_in[...]
        old = m_ref[t]
        new = jnp.maximum(old, jnp.max(sc, axis=0, keepdims=True))
        p = jnp.exp2((sc - new) * LOG2E)
        scale = jnp.exp2((old - new) * LOG2E)
        l_ref[t] = l_ref[t] * scale + jnp.sum(p.reshape(16, 8, 512), axis=0)
        m_ref[t] = new
        p_out[...] = p.astype(BF)
        a_out[...] = scale

    def add_values(t, p_in, a_in):
        s, j = t % 2, t // 2
        for h in range(2):
            vals = vbuf[j * 128 + h * 64 : j * 128 + h * 64 + 64, s * 128 : s * 128 + 128]
            lanes = slice(h * 256, h * 256 + 256)
            acc[2 * t + h] = acc[2 * t + h] * a_in[:, lanes] + dot(vals, p_in[:, lanes], NN)

    def attend(order, hooks):
        def weigh_step(i):
            weigh(order[i], s_b[i % AHEAD], p_b[i % (LAG + 1)], a_b[i % (LAG + 1)])

        for i in range(AHEAD):
            scores(order[i], s_b[i])
        for i in range(LAG):
            weigh_step(i)
        for i, t in enumerate(order):
            if i + LAG < STEPS:
                weigh_step(i + LAG)
            if i + AHEAD < STEPS:
                scores(order[i + AHEAD], s_b[i % AHEAD])
            add_values(t, p_b[i % (LAG + 1)], a_b[i % (LAG + 1)])
            if i in hooks:
                hooks[i]()

    def pass_on(b, c):
        for s in range(2):
            arrived_part(b, s, c).wait_recv()
            relay_part(b, s, c).start()

    def whole_block(b):
        @pl.when(b >= 2)
        def _():
            for s in range(2):
                relay(b, s).wait_recv()

        for n in range(2):
            kbuf[:, n * 512 : n * 512 + 512] = dot(xbuf[b], wk[n * 512 : n * 512 + 512, :], NT).astype(BF)
        for n in range(2):
            vbuf[n * 512 : n * 512 + 512, :] = dot(wv[n * 512 : n * 512 + 512, :], xbuf[b], NT).astype(BF)

        @pl.when((b >= 1) & (b < FIRST_PART - 1))
        def _():
            for s in range(2):
                arrived(b + 1, s).wait_recv()
                relay(b + 1, s).start()

        @pl.when((b >= 1) & (b < 3))
        def _():
            for c in range(PARTS):
                for s in range(2):
                    forward_part(b + 1, s, c).start()

        @pl.when(b == FIRST_PART - 1)
        def _():
            pass_on(FIRST_PART, 0)

    def project_part(b, c):
        cols = slice(COLS[c], COLS[c + 1])
        x_part = xbuf[b, :, cols]
        for n in range(2):
            lanes = slice(n * 512, n * 512 + 512)
            k_new = dot(x_part, wk[lanes, cols], NT)
            v_new = dot(wv[lanes, cols], x_part, NT)
            if c > 0:
                k_new += k_acc[:, lanes]
                v_new += v_acc[lanes, :]
            if c < PARTS - 1:
                k_acc[:, lanes] = k_new
                v_acc[lanes, :] = v_new
            else:
                kbuf[:, lanes] = k_new.astype(BF)
                vbuf[lanes, :] = v_new.astype(BF)

    def part_block(b):
        for c in range(PARTS):
            if c + 1 < PARTS:
                pass_on(b, c + 1)
            for s in range(2):
                relay_part(b, s, c).wait_recv()
            project_part(b, c)

    def block(b, carry):
        @pl.when(b < FIRST_PART)
        def _():
            whole_block(b)

        @pl.when(b >= FIRST_PART)
        def _():
            part_block(b)
            pass_on(b + 1, 0)

        attend(list(range(STEPS)), {})
        return carry

    lax.fori_loop(0, BLOCKS - 1, block, 0)
    part_block(BLOCKS - 1)

    def o_copy(s):
        dst = o_buf.at[pl.ds(s * 128, 128), pl.ds(HALF, HALF)]
        return remote(o_out.at[pl.ds(s * 128, 128)], dst, o_send.at[s], o_recv.at[s], mate)

    def finish(s):
        for j in range(PAIRS):
            t = 2 * j + s
            total = jnp.sum(l_ref[t], axis=0, keepdims=True)
            parts = [acc[2 * t + h] / total[:, h * 256 : h * 256 + 256] for h in range(2)]
            o_rows = jnp.concatenate(parts, axis=0).T.astype(BF)
            o_out[s * 128 : s * 128 + 128, j * 128 : j * 128 + 128] = o_rows[128:]
            o_buf[s * 128 : s * 128 + 128, j * 128 : j * 128 + 128] = o_rows[:128]
        o_copy(s).start()

    for c in wo_copies:
        c.wait()

    def other_share(s, n):
        rows, lanes = slice(s * 128, s * 128 + 128), slice(n * 512, n * 512 + 512)
        y_ref[rows, lanes] = (y_acc[rows, lanes] + dot(o_buf[rows, HALF:], wo[HALF:, lanes], NN)).astype(BF)

    attend([2 * j + s for s in range(2) for j in range(PAIRS)], {PAIRS - 1: lambda: finish(0)})
    finish(1)
    for n in range(4):
        lanes = slice(n * 512, n * 512 + 512)
        y_acc[:, lanes] = dot(o_buf[:, :HALF], wo[:HALF, lanes], NN)
    for s in range(2):
        o_copy(s).wait_recv()
        for n in range(4):
            other_share(s, n)

    to_mate.wait_send()
    for c in sends:
        c.wait_send()
    for s in range(2):
        o_copy(s).wait_send()
        for b in range(2, FIRST_PART):
            relay(b, s).wait_send()
        for c in range(PARTS):
            for b in range(2, 4):
                forward_part(b, s, c).wait_send()
            for b in range(FIRST_PART, BLOCKS):
                relay_part(b, s, c).wait_send()


def solution(mesh):
    tok_spec = P("data", ("row", "col", "core"), None)

    def per_device(tokens, w_qkv, w_out):
        x = tokens.reshape(256, 2048)
        wt = jnp.transpose(w_qkv, (1, 2, 3, 0)).reshape(6144, 2048)
        wo = w_out.reshape(2048, 2048)
        dma = pltpu.SemaphoreType.DMA
        local = [
            pltpu.VMEM((STEPS, 128, 512), BF),
            pltpu.VMEM((256, HALF), BF),
            pltpu.VMEM((HALF, 256), BF),
            *[pltpu.VMEM((128, 512), F32)] * AHEAD,
            *[pltpu.VMEM((128, 512), BF)] * (LAG + 1),
            *[pltpu.VMEM((1, 512), F32)] * (LAG + 1),
        ]
        y = pl.pallas_call(
            lambda *refs: pl.run_scoped(functools.partial(kernel, *refs), *local),
            out_shape=jax.ShapeDtypeStruct((256, 2048), BF),
            in_specs=[pl.BlockSpec(memory_space=pl.ANY)] * 3,
            out_specs=pl.BlockSpec(memory_space=pltpu.VMEM),
            scratch_shapes=[
                pltpu.VMEM((BLOCKS, 256, 2048), BF),
                pltpu.VMEM((HALF, 2048), BF),
                pltpu.VMEM((HALF, 2048), BF),
                pltpu.VMEM((HALF, 2048), BF),
                pltpu.VMEM((2048, 2048), BF),
                pltpu.VMEM((256, HALF), F32),
                pltpu.VMEM((HALF, 256), F32),
                pltpu.VMEM((2 * STEPS, 64, 256), F32),
                pltpu.VMEM((STEPS, 1, 512), F32),
                pltpu.VMEM((STEPS, 8, 512), F32),
                pltpu.VMEM((256, 2048), BF),
                pltpu.VMEM((256, HALF), BF),
                pltpu.VMEM((256, 2048), F32),
                dma((14,)),
                dma((4,)),
                dma,
                dma,
                dma((FIRST_PART, 2)),
                dma((FIRST_PART, 2)),
                dma((FIRST_PART, 2)),
                dma((FIRST_PART, 2)),
                dma((BLOCKS - FIRST_PART, 2, PARTS)),
                dma((BLOCKS - FIRST_PART, 2, PARTS)),
                dma((BLOCKS - FIRST_PART, 2, PARTS)),
                dma((BLOCKS - FIRST_PART, 2, PARTS)),
                dma((2,)),
                dma((2,)),
            ],
            compiler_params=pltpu.CompilerParams(
                collective_id=0, has_side_effects=True, vmem_limit_bytes=52 * 1024 * 1024
            ),
            name="attention",
        )(x, wt, wo)
        return y.reshape(2, 128, 2048)

    return jax.shard_map(per_device, mesh=mesh, in_specs=(tok_spec, P(), P()), out_specs=tok_spec, check_vma=False)
```
